32 devices in a mesh: dp: 8 (over z, x), feat: 4 (over y, core).
Axes of the slice: x: 2, y: 2, z: 4, core: 2. Of those that a mesh axis runs over, the one named last changes fastest.
Arguments:
- tokens: bfloat16 [8192, 768], P(('dp', 'feat')), may hold values from -11 to 11
- lengths: int32 [8, 2], replicated, may hold values from 0 to 1024, as said below
- joint_weight: bfloat16 [768, 2304], replicated, may hold values from -0.21875 to 0.21875
- joint_bias: float32 [2304], replicated, may hold values from -17.5 to 17.5
- output_weight: bfloat16 [768, 768], replicated, may hold values from -1.75 to 1.75
- output_bias: float32 [768], replicated, may hold values from -2.4 to 2.4
- first_gain: float32 [768], replicated, may hold values from 0.5 to 1.5
- first_shift: float32 [768], replicated, may hold values from -1 to 1
- up_weight: bfloat16 [768, 3072], replicated, may hold values from -0.21875 to 0.21875
- up_bias: float32 [3072], replicated, may hold values from -1 to 1
- down_weight: bfloat16 [3072, 768], replicated, may hold values from -0.109375 to 0.109375
- down_bias: float32 [768], replicated, may hold values from -1 to 1
- second_gain: float32 [768], replicated, may hold values from 0.5 to 1.5
- second_shift: float32 [768], replicated, may hold values from -1 to 1
- feature_matrix: bfloat16 [12, 256, 64], P(None, 'feat'), may hold values from -6 to 6
- cotangent: bfloat16 [8192, 768], P(('dp', 'feat')), may hold values from -6 to 6
Outputs:
- layer_output: bfloat16 [8192, 768], P(('dp', 'feat'))
- input_gradient: float32 [8192, 768], P(('dp', 'feat'))
- grad_joint: float32 [768, 2304], P(('dp', 'feat'))
- grad_jointbias: float32 [2304], P(('dp', 'feat'))
- grad_output: float32 [768, 768], P(('dp', 'feat'))
- grad_outputbias: float32 [768], P(('dp', 'feat'))
- grad_firstgain: float32 [768], P(('dp', 'feat'))
- grad_firstshift: float32 [768], P(('dp', 'feat'))
- grad_up: float32 [768, 3072], P(('dp', 'feat'))
- grad_upbias: float32 [3072], P(('dp', 'feat'))
- grad_down: float32 [3072, 768], P(('dp', 'feat'))
- grad_downbias: float32 [768], P(('dp', 'feat'))
- grad_secondgain: float32 [768], P(('dp', 'feat'))
- grad_secondshift: float32 [768], P(('dp', 'feat'))
- token_moments: float32 [3], replicated
The draws below stay inside these ranges and needn't reach their ends.
Inputs may be any that keep to these rules, and one draw needn't show every extreme that they name: In each row the nonzero lengths come first, each 1024 or more, and they add up to at most 1024; some row holds one sequence of 1024 tokens.
All inputs are finite; a program needn't handle non-finite values.
Results may differ from the reference program's by a relative error of at most 0.035.
Values may be sent and summed in bfloat16 or wider, within the bound.
A program may use at most 192 MiB of HBM per device.

```python
import jax
import jax.numpy as jnp
from jax import lax

H = 12
DH = 64
D = 768
FF = 3072
M = 256
MINLEN = 1024
NSEG = 2
ROW = 1024
ROWS = 8
TOKENS = 8192


def draw_tokens(key, part):
    entries = jnp.clip(jax.random.normal(key, (TOKENS, D), jnp.float32), -6.0, 6.0)
    rising = jnp.sqrt(1.0 + 2.0 * jnp.arange(TOKENS).astype(jnp.float32) / TOKENS)
    return (entries * rising[:, None]).astype(jnp.bfloat16)


def draw_feature_matrix(key, part):
    entries = jnp.clip(jax.random.normal(jax.random.fold_in(key, 3), (H, M, DH), jnp.float32), -4.0, 4.0)
    return entries.astype(jnp.bfloat16)


def draw_joint_bias(key, part):
    entries = jnp.clip(0.2 * jax.random.normal(jax.random.fold_in(key, 17), (3 * D,), jnp.float32), -1.0, 1.0)
    return entries


def draw_lengths(key, part):
    room_span = ROW - MINLEN
    subkeys = jax.random.split(key, NSEG + 3)
    first_draw = jax.random.randint(subkeys[0], (ROWS,), 0, room_span + 1)
    second_draw = jax.random.randint(subkeys[1], (ROWS,), 0, room_span + 1)
    first_length = MINLEN + first_draw * second_draw // max(room_span, 1)
    full_row = jax.random.randint(subkeys[2], (), 0, ROWS)
    first_length = jnp.where(jnp.arange(ROWS).astype(jnp.int32) == full_row, ROW, first_length)
    columns = [first_length]
    used_tokens = first_length
    for segment in range(1, NSEG):
        remaining = ROW - used_tokens
        raw_draw = jax.random.randint(subkeys[2 + segment], (ROWS,), 0, 1 << 20)
        extra_tokens = raw_draw % jnp.maximum(remaining - MINLEN + 1, 1)
        seq_length = jnp.where(remaining >= MINLEN, MINLEN + extra_tokens, 0)
        columns.append(seq_length)
        used_tokens = used_tokens + seq_length
    return jnp.stack(columns, 1).astype(jnp.int32)


def block_levels(stream_key, extent, cuts, low, top_value):
    gain, own = 1.0, jax.random.fold_in(stream_key, 6)
    for axis_at, parts in cuts:
        heights = jnp.exp(jax.random.uniform(jax.random.fold_in(own, axis_at), (parts,), jnp.float32, low / len(cuts), top_value / len(cuts)))
        gain = gain * jnp.repeat(heights, extent[axis_at] // parts).reshape([-1 if axis == axis_at else 1 for axis in range(len(extent))])
    return gain


def gaussian(rng, shape, deviation, reach, pieces=(), kind=jnp.bfloat16):
    values = jax.random.normal(rng, shape, jnp.float32) * deviation
    if len(pieces) > 0:
        values = block_levels(rng, shape, pieces, -0.22, 0.18) * values
    return jnp.clip(values, min=-reach, max=reach).astype(kind)


def setup_inputs(seed: int = 0) -> dict:
    key_of = jax.random.split(jax.random.key(seed), 17)
    tokens = draw_tokens(jax.random.fold_in(key_of[16], 71), 0)
    lengths = draw_lengths(jax.random.fold_in(key_of[16], 71), 0)
    joint_weight = gaussian(key_of[2], (D, 3 * D), D ** -0.5, 0.21875)
    joint_bias = draw_joint_bias(jax.random.fold_in(key_of[16], 71), 0)
    output_weight = gaussian(key_of[4], (D, D), (D // 64) ** -0.5, 1.75)
    output_bias = gaussian(key_of[5], (D,), 0.6, 2.4, (), jnp.float32)
    first_gain = jnp.clip(1.0 + 0.1 * jax.random.normal(key_of[6], (D,), jnp.float32), 0.5, 1.5)
    first_shift = gaussian(key_of[7], (D,), 0.2, 1.0, (), jnp.float32)
    up_weight = gaussian(key_of[8], (D, FF), D ** -0.5, 0.21875)
    up_bias = gaussian(key_of[9], (FF,), 0.2, 1.0, (), jnp.float32)
    down_weight = gaussian(key_of[10], (FF, D), FF ** -0.5, 0.109375)
    down_bias = gaussian(key_of[11], (D,), 0.2, 1.0, (), jnp.float32)
    second_gain = jnp.clip(1.0 + 0.1 * jax.random.normal(key_of[12], (D,), jnp.float32), 0.5, 1.5)
    second_shift = gaussian(key_of[13], (D,), 0.2, 1.0, (), jnp.float32)
    feature_matrix = draw_feature_matrix(jax.random.fold_in(key_of[16], 71), 0)
    cotangent = gaussian(key_of[15], (TOKENS, D), 1.0, 6.0, ((0, 32),))
    return {"tokens": tokens, "lengths": lengths, "joint_weight": joint_weight, "joint_bias": joint_bias, "output_weight": output_weight, "output_bias": output_bias, "first_gain": first_gain, "first_shift": first_shift, "up_weight": up_weight, "up_bias": up_bias, "down_weight": down_weight, "down_bias": down_bias, "second_gain": second_gain, "second_shift": second_shift, "feature_matrix": feature_matrix, "cotangent": cotangent}


@jax.custom_vjp
def low(v):
    return lax.optimization_barrier(v.astype(jnp.bfloat16)).astype(jnp.float32)

@jax.custom_vjp
def low_back(v):
    return v

def low_keep(v):
    return (low(v), None)

def low_pass(kept, grad):
    return (grad,)

def back_keep(v):
    return (v, None)

def back_low(kept, grad):
    return (low(grad),)
low.defvjp(low_keep, low_pass)
low_back.defvjp(back_keep, back_low)
epsilon = 1e-06

def layer_norm(residual, scaling, offset):
    center = residual - lax.optimization_barrier(jnp.mean(residual, -1, keepdims=True))
    spread = lax.optimization_barrier(jnp.mean(center * center, -1, keepdims=True))
    return center * lax.rsqrt(spread + epsilon) * scaling + offset

def forward(tokens_row, params, projection_matrix, segment_ids, valid_mask):
    joint_weight, joint_bias, output_weight, output_bias, first_gain, first_shift, up_weight, up_bias, down_weight, down_bias, second_gain, second_shift = params
    highest_precision = lax.Precision.HIGHEST
    score_scale_factor = DH ** (-0.25)
    joint_rows = low(low_back(jnp.dot(tokens_row, joint_weight, precision=highest_precision) + joint_bias))
    query_matrix = joint_rows[:, :D].reshape(ROW, H, DH)
    key_token_row = joint_rows[:, D:2 * D].reshape(ROW, H, DH)
    values_row = joint_rows[:, 2 * D:].reshape(ROW, H, DH)
    query_feature_scores = low_back(score_scale_factor * jnp.einsum('bjv,jsv->bjs', query_matrix, projection_matrix, precision=highest_precision))
    key_feature_scores = low_back(score_scale_factor * jnp.einsum('bjv,jsv->bjs', key_token_row, projection_matrix, precision=highest_precision))
    query_sq = score_scale_factor * score_scale_factor * lax.optimization_barrier(jnp.sum(query_matrix * query_matrix, -1)) / 2
    key_sq = score_scale_factor * score_scale_factor * lax.optimization_barrier(jnp.sum(key_token_row * key_token_row, -1)) / 2
    valid_cube = valid_mask[:, None, None]
    query_shift = query_feature_scores - query_sq[..., None]
    key_shift = key_feature_scores - key_sq[..., None]
    query_top = lax.optimization_barrier(jnp.max(query_shift, -1))
    key_top = lax.optimization_barrier(jnp.max(jnp.where(valid_cube > 0, key_shift, -1e+30), axis=(0, 2)))
    query_feature_maps = low(jnp.exp(query_shift - query_top[..., None]) * M ** (-0.5))
    key_feats = low(jnp.exp(key_shift - key_top[None, :, None]) * M ** (-0.5) * valid_cube)
    member = (segment_ids[None, :] == jnp.arange(NSEG).astype(jnp.int32)[:, None]).astype(jnp.float32)
    padded_key_rows = member[:, :, None, None] * key_feats[None]
    sequence_key_state = low(low_back(jnp.einsum('sthm,thd->shmd', padded_key_rows, values_row, precision=highest_precision)))
    totals = lax.optimization_barrier(jnp.sum(padded_key_rows, axis=1))
    padded_query_rows = member[:, :, None, None] * query_feature_maps[None]
    numerator = jnp.einsum('sthm,shmd->thd', padded_query_rows, sequence_key_state, precision=highest_precision)
    denominator = jnp.einsum('sthm,shm->th', padded_query_rows, totals, precision=highest_precision)
    padding = 1.0 - valid_mask
    safe_denom = low_back(denominator) + padding[:, None]
    attention = low(low_back(numerator) / safe_denom[..., None]).reshape(ROW, D)
    branch_attn = low_back(jnp.dot(attention, output_weight, precision=highest_precision) + output_bias)
    hidden = layer_norm(tokens_row + branch_attn, first_gain, first_shift)
    pre_act = low_back(jnp.dot(low(hidden), up_weight, precision=highest_precision) + up_bias)
    activated = low(jax.nn.gelu(pre_act, approximate=False))
    branch_ffn = low_back(jnp.dot(activated, down_weight, precision=highest_precision) + down_bias)
    result = layer_norm(hidden + branch_ffn, second_gain, second_shift) * valid_mask[:, None]
    moments = jnp.stack([jnp.sum(valid_mask * lax.optimization_barrier(jnp.sum(tokens_row * tokens_row, -1))), jnp.sum(valid_mask * lax.optimization_barrier(jnp.sum(branch_attn * branch_attn, -1))), jnp.sum(valid_mask * lax.optimization_barrier(jnp.sum(branch_ffn * branch_ffn, -1)))])
    return (result, moments)

def reference(tokens, lengths, joint_weight, joint_bias, output_weight, output_bias, first_gain, first_shift, up_weight, up_bias, down_weight, down_bias, second_gain, second_shift, feature_matrix, cotangent):
    params = tuple((entry.astype(jnp.float32) for entry in (joint_weight, joint_bias, output_weight, output_bias, first_gain, first_shift, up_weight, up_bias, down_weight, down_bias, second_gain, second_shift)))
    projection_matrix = feature_matrix.astype(jnp.float32)
    rows_in = tokens.astype(jnp.float32).reshape(ROWS, ROW, D)
    rows_back = cotangent.astype(jnp.float32).reshape(ROWS, ROW, D)

    def one_row(running, entries):
        tokens_row, lengths_row, cot_row = entries
        seq_ends = jnp.cumsum(lengths_row).astype(jnp.int32)
        positions = jnp.arange(ROW).astype(jnp.int32)
        segment_ids = lax.optimization_barrier(jnp.sum((positions[:, None] >= seq_ends[None, :]).astype(jnp.int32), axis=1)).astype(jnp.int32)
        valid_mask = (positions < seq_ends[NSEG - 1]).astype(jnp.float32)

        def layer_apply(input_value_rows, weights_in):
            return forward(input_value_rows, weights_in, projection_matrix, segment_ids, valid_mask)
        result, pullback, moments = jax.vjp(layer_apply, tokens_row, params, has_aux=True)
        token_grad, weight_grads = pullback(cot_row)
        grad_sums, moment_sums, valid_count = running
        grad_sums = jax.tree.map(jnp.add, grad_sums, weight_grads)
        return ((grad_sums, moment_sums + moments, valid_count + jnp.sum(valid_mask)), (result.astype(jnp.bfloat16), token_grad))
    initial = (jax.tree.map(jnp.zeros_like, params), jnp.zeros((3,), jnp.float32), jnp.zeros((), jnp.float32))
    (grad_sums, moment_sums, valid_count), (outputs, token_grads) = lax.scan(one_row, initial, (rows_in, lengths, rows_back))
    token_moments = jnp.sqrt(moment_sums / (valid_count * D))
    return (outputs.reshape(ROWS * ROW, D), token_grads.reshape(ROWS * ROW, D), grad_sums[0], grad_sums[1], grad_sums[2], grad_sums[3], grad_sums[4], grad_sums[5], grad_sums[6], grad_sums[7], grad_sums[8], grad_sums[9], grad_sums[10], grad_sums[11], token_moments)
```

```python
import jax
import jax.numpy as jnp
from jax import lax
from jax.sharding import PartitionSpec as P

epsilon = 1e-06
f32 = jnp.float32
bf16 = jnp.bfloat16


def mm(spec, a, b):
    return jnp.einsum(spec, a, b, preferred_element_type=f32)


def layer_norm_parts(v):
    center = v - jnp.mean(v, -1, keepdims=True)
    inv = lax.rsqrt(jnp.mean(center * center, -1, keepdims=True) + epsilon)
    return center * inv, inv


def layer_norm_back(grad, normal, inv, gain):
    scaled = grad * gain
    return inv * (
        scaled
        - jnp.mean(scaled, -1, keepdims=True)
        - normal * jnp.mean(scaled * normal, -1, keepdims=True)
    )


def attention_forward(qkv, features, valid, heads, size):
    rows = qkv.shape[0]
    model = heads * size
    scale = size ** (-0.25)
    norm = features.shape[1] ** (-0.5)
    q, k, v = (
        qkv[:, i * model : (i + 1) * model].reshape(rows, heads, size).transpose(1, 0, 2)
        for i in range(3)
    )
    qw, kw = q.astype(f32), k.astype(f32)
    q_shift = scale * mm("htd,hmd->htm", q, features) - (
        scale * scale / 2 * jnp.sum(qw * qw, -1, keepdims=True)
    )
    k_shift = scale * mm("htd,hmd->htm", k, features) - (
        scale * scale / 2 * jnp.sum(kw * kw, -1, keepdims=True)
    )
    q_top = jnp.max(q_shift, -1, keepdims=True)
    k_top = lax.pmax(jnp.max(k_shift, axis=(1, 2)), "feat")[:, None, None]
    q_raw = jnp.exp(q_shift - q_top) * norm
    k_raw = jnp.exp(k_shift - k_top) * norm * valid
    q_feat, k_feat = q_raw.astype(bf16), k_raw.astype(bf16)
    state = lax.psum(mm("htm,htd->hmd", k_feat, v), "feat").astype(bf16)
    totals = lax.psum(jnp.sum(k_feat.astype(f32), 1), "feat")
    numer = mm("htm,hmd->htd", q_feat, state) * valid
    denom = jnp.sum(q_feat.astype(f32) * totals[:, None, :], -1, keepdims=True) * valid
    safe = denom + (1.0 - valid)
    attention = (numer / safe).astype(bf16).transpose(1, 0, 2).reshape(rows, model)
    return attention, (q, k, v, q_raw, k_raw, state, totals, numer, safe)


def attention_backward(g_att, saved, features, valid, heads, size):
    q, k, v, q_raw, k_raw, state, totals, numer, safe = saved
    rows = g_att.shape[0]
    scale = size ** (-0.25)
    g_att = g_att.reshape(rows, heads, size).transpose(1, 0, 2)
    q_feat, k_feat = q_raw.astype(bf16), k_raw.astype(bf16)
    g_num = (g_att / safe * valid).astype(bf16)
    g_den = (-jnp.sum(g_att * numer, -1, keepdims=True) / (safe * safe) * valid).astype(bf16)
    g_den = g_den.astype(f32)
    g_state = lax.psum(mm("htm,htd->hmd", q_feat, g_num), "feat").astype(bf16)
    g_totals = lax.psum(jnp.sum(q_feat.astype(f32) * g_den, 1), "feat")
    g_aq = (mm("htd,hmd->htm", g_num, state) + g_den * totals[:, None, :]) * q_raw
    g_ak = (mm("htd,hmd->htm", v, g_state) + g_totals[:, None, :]) * k_raw
    g_v = mm("htm,hmd->htd", k_feat, g_state)

    def back(g_a, x):
        return scale * mm("htm,hmd->htd", g_a.astype(bf16), features) - (
            scale * scale * x.astype(f32) * jnp.sum(g_a, -1, keepdims=True)
        )

    parts = [back(g_aq, q), back(g_ak, k), g_v]
    return jnp.concatenate(
        [p.astype(bf16).transpose(1, 0, 2).reshape(rows, heads * size) for p in parts], axis=1
    )


def on_device(
    tokens,
    lengths,
    joint_weight,
    joint_bias,
    output_weight,
    output_bias,
    first_gain,
    first_shift,
    up_weight,
    up_bias,
    down_weight,
    down_bias,
    second_gain,
    second_shift,
    feature_matrix,
    cotangent,
):
    model = tokens.shape[1]
    heads, _, size = feature_matrix.shape
    both = ("dp", "feat")
    row_lengths = lax.dynamic_index_in_dim(lengths, lax.axis_index("dp"), 0, keepdims=False)
    valid = (row_lengths[0] > 0).astype(f32)
    features = lax.all_gather(feature_matrix, "feat", axis=1, tiled=True)
    qkv = (mm("td,de->te", tokens, joint_weight) + joint_bias).astype(bf16)
    attention, saved = attention_forward(qkv, features, valid, heads, size)
    branch_attn = mm("td,de->te", attention, output_weight) + output_bias
    wide = tokens.astype(f32)
    normal_1, inv_1 = layer_norm_parts(wide + branch_attn)
    hidden = normal_1 * first_gain + first_shift
    hidden_low = hidden.astype(bf16)
    pre = mm("td,df->tf", hidden_low, up_weight) + up_bias
    half_erf = 0.5 * (1.0 + lax.erf(pre * (0.5**0.5)))
    slope = half_erf + pre * jnp.exp(-0.5 * pre * pre) * 0.3989422804014327
    activated = (pre * half_erf).astype(bf16)
    branch_ffn = mm("tf,fd->td", activated, down_weight) + down_bias
    normal_2, inv_2 = layer_norm_parts(hidden + branch_ffn)
    layer_output = ((normal_2 * second_gain + second_shift) * valid).astype(bf16)
    moments = valid * jnp.stack(
        [jnp.sum(wide * wide), jnp.sum(branch_attn * branch_attn), jnp.sum(branch_ffn * branch_ffn)]
    )
    g_out = cotangent.astype(f32) * valid
    grad_secondgain = jnp.sum(g_out * normal_2, 0)
    grad_secondshift = jnp.sum(g_out, 0)
    g_second = layer_norm_back(g_out, normal_2, inv_2, second_gain)
    g_ffn = g_second.astype(bf16)
    grad_down = mm("tf,td->fd", activated, g_ffn)
    grad_downbias = jnp.sum(g_ffn.astype(f32), 0)
    g_pre = (mm("td,fd->tf", g_ffn, down_weight) * slope).astype(bf16)
    grad_up = mm("td,tf->df", hidden_low, g_pre)
    grad_upbias = jnp.sum(g_pre.astype(f32), 0)
    g_hidden = g_second + mm("tf,df->td", g_pre, up_weight)
    grad_firstgain = jnp.sum(g_hidden * normal_1, 0)
    grad_firstshift = jnp.sum(g_hidden, 0)
    g_first = layer_norm_back(g_hidden, normal_1, inv_1, first_gain)
    g_branch = g_first.astype(bf16)
    grad_output = mm("td,te->de", attention, g_branch)
    grad_outputbias = jnp.sum(g_branch.astype(f32), 0)
    g_att = mm("te,de->td", g_branch, output_weight)
    g_qkv = attention_backward(g_att, saved, features, valid, heads, size)
    grad_joint = mm("td,te->de", tokens, g_qkv)
    grad_jointbias = jnp.sum(g_qkv.astype(f32), 0)
    input_gradient = g_first + mm("te,de->td", g_qkv, joint_weight)

    shards = lax.axis_size(both)
    small = jnp.concatenate(
        [
            p.reshape(shards, -1)
            for p in (
                grad_jointbias,
                grad_outputbias,
                grad_firstgain,
                grad_firstshift,
                grad_upbias,
                grad_downbias,
                grad_secondgain,
                grad_secondshift,
            )
        ]
        + [jnp.broadcast_to(moments, (shards, 3))],
        axis=1,
    )
    small = lax.psum_scatter(small, both, scatter_dimension=0, tiled=True)[0]
    each = model // shards
    cuts, at = [], 0
    for width in (3 * each, each, each, each, up_bias.shape[0] // shards, each, each, each, 3):
        cuts.append(small[at : at + width])
        at += width

    def scatter(partial):
        return lax.psum_scatter(
            partial.astype(bf16), both, scatter_dimension=0, tiled=True
        ).astype(f32)

    valid_count = jnp.sum(lengths).astype(f32)
    token_moments = jnp.sqrt(cuts[8] / (valid_count * model))
    return (
        layer_output,
        input_gradient,
        scatter(grad_joint),
        cuts[0],
        scatter(grad_output),
        cuts[1],
        cuts[2],
        cuts[3],
        scatter(grad_up),
        cuts[4],
        scatter(grad_down),
        cuts[5],
        cuts[6],
        cuts[7],
        token_moments,
    )


def solution(mesh):
    rows = P(("dp", "feat"), None)
    flat = P(("dp", "feat"))
    in_specs = (rows,) + (P(),) * 13 + (P(None, "feat", None), rows)
    out_specs = (rows, rows, rows, flat, rows, flat, flat, flat, rows, flat, rows, flat, flat, flat, P())
    return jax.shard_map(
        on_device, mesh=mesh, in_specs=in_specs, out_specs=out_specs, check_vma=False
    )
```

```python
import functools

import jax
import jax.numpy as jnp
from jax import lax
from jax.experimental import pallas as pl
from jax.experimental.pallas import tpu as pltpu
from jax.sharding import PartitionSpec as P

epsilon = 1e-06
f32 = jnp.float32
bf16 = jnp.bfloat16


def mm(spec, a, b):
    return jnp.einsum(spec, a, b, preferred_element_type=f32)


def layer_norm_parts(v):
    center = v - jnp.mean(v, -1, keepdims=True)
    inv = lax.rsqrt(jnp.mean(center * center, -1, keepdims=True) + epsilon)
    return center * inv, inv


def layer_norm_back(grad, normal, inv, gain):
    scaled = grad * gain
    return inv * (
        scaled
        - jnp.mean(scaled, -1, keepdims=True)
        - normal * jnp.mean(scaled * normal, -1, keepdims=True)
    )


def attention_forward(qkv, features, valid, heads, size):
    rows = qkv.shape[0]
    model = heads * size
    scale = size ** (-0.25)
    norm = features.shape[1] ** (-0.5)
    q, k, v = (
        qkv[:, i * model : (i + 1) * model].reshape(rows, heads, size).transpose(1, 0, 2)
        for i in range(3)
    )
    qw, kw = q.astype(f32), k.astype(f32)
    q_shift = scale * mm("htd,hmd->htm", q, features) - (
        scale * scale / 2 * jnp.sum(qw * qw, -1, keepdims=True)
    )
    k_shift = scale * mm("htd,hmd->htm", k, features) - (
        scale * scale / 2 * jnp.sum(kw * kw, -1, keepdims=True)
    )
    q_top = jnp.max(q_shift, -1, keepdims=True)
    k_top = lax.pmax(jnp.max(k_shift, axis=(1, 2)), "feat")[:, None, None]
    q_raw = jnp.exp(q_shift - q_top) * norm
    k_raw = jnp.exp(k_shift - k_top) * norm * valid
    q_feat, k_feat = q_raw.astype(bf16), k_raw.astype(bf16)
    state = lax.psum(mm("htm,htd->hmd", k_feat, v), "feat").astype(bf16)
    totals = lax.psum(jnp.sum(k_feat.astype(f32), 1), "feat")
    numer = mm("htm,hmd->htd", q_feat, state) * valid
    denom = jnp.sum(q_feat.astype(f32) * totals[:, None, :], -1, keepdims=True) * valid
    safe = denom + (1.0 - valid)
    attention = (numer / safe).astype(bf16).transpose(1, 0, 2).reshape(rows, model)
    return attention, (q, k, v, q_raw, k_raw, state, totals, numer, safe)


def attention_backward(g_att, saved, features, valid, heads, size):
    q, k, v, q_raw, k_raw, state, totals, numer, safe = saved
    rows = g_att.shape[0]
    scale = size ** (-0.25)
    g_att = g_att.reshape(rows, heads, size).transpose(1, 0, 2)
    q_feat, k_feat = q_raw.astype(bf16), k_raw.astype(bf16)
    g_num = (g_att / safe * valid).astype(bf16)
    g_den = (-jnp.sum(g_att * numer, -1, keepdims=True) / (safe * safe) * valid).astype(bf16)
    g_den = g_den.astype(f32)
    g_state = lax.psum(mm("htm,htd->hmd", q_feat, g_num), "feat").astype(bf16)
    g_totals = lax.psum(jnp.sum(q_feat.astype(f32) * g_den, 1), "feat")
    g_aq = (mm("htd,hmd->htm", g_num, state) + g_den * totals[:, None, :]) * q_raw
    g_ak = (mm("htd,hmd->htm", v, g_state) + g_totals[:, None, :]) * k_raw
    g_v = mm("htm,hmd->htd", k_feat, g_state)

    def back(g_a, x):
        return scale * mm("htm,hmd->htd", g_a.astype(bf16), features) - (
            scale * scale * x.astype(f32) * jnp.sum(g_a, -1, keepdims=True)
        )

    parts = [back(g_aq, q), back(g_ak, k), g_v]
    return jnp.concatenate(
        [p.astype(bf16).transpose(1, 0, 2).reshape(rows, heads * size) for p in parts], axis=1
    )


MESH = pl.DeviceIdType.MESH


class Chunk:
    def __init__(self, part, first, r, w, kind, bufs, sems):
        self.part, self.first, self.r, self.w, self.kind = part, first, r, w, kind
        self.b1, self.b2, self.b3, self.fin, self.got = bufs
        self.sems = sems


def plan(tokens, joint, up):
    half_joint, half_up, half = joint // 2, up // 2, tokens // 2
    return (
        ("up", half_up // 3, 3),
        ("down", half // 3, 3),
        ("output", half, 1),
        ("joint", half_joint // 3, 3),
    )


def scatter_kernel(chips, model, *refs):
    (tok, att, hid, act, g_qkv, g_branch, g_pre, g_ffn, small) = refs[:9]
    outs = dict(zip(("joint", "output", "up", "down", "small"), refs[9:14]))
    scratch = list(refs[14:])
    pair = dict(zip(("tok", "att", "hid", "act", "qkv", "branch", "pre", "ffn", "small"), scratch[:9]))
    parts = dict(zip(("up", "down", "output", "joint", "small"), scratch[9:14]))
    pair_send, pair_recv, send, recv = scratch[14:18]
    rest = scratch[18:]

    dp, feat = lax.axis_index("dp"), lax.axis_index("feat")
    depth = chips // 4
    z, x, y, c = dp // 2, dp % 2, feat // 2, feat % 2
    core = (dp, y * 2 + 1 - c)

    def route(turn):
        return (
            (x + turn * (y - x), 2 - turn),
            (y + turn * (x - y), 1 + turn),
            (z * 2 + x + (1 - turn) * (1 - 2 * x), (y + turn * (1 - 2 * y)) * 2 + c),
            (z * 2 + x + turn * (1 - 2 * x), (y + (1 - turn) * (1 - 2 * y)) * 2 + c),
        )

    routes = {False: route(c), True: route(0)}

    def along(k):
        return ((z + k) % depth * 2 + x, feat)

    barrier = pltpu.get_barrier_semaphore()
    greeted = [core, *routes[False][2:]] + [along(k) for k in range(1, depth)]
    for device in greeted:
        pl.semaphore_signal(barrier, inc=1, device_id=device, device_id_type=MESH)
    pl.semaphore_wait(barrier, len(greeted))

    def halves(ref):
        width = ref.shape[1] // 2
        return ref.at[:, pl.ds(pl.multiple_of((1 - c) * width, 128), width)]

    exchange = []
    sources = (
        ("small", small.at[:, 1 - c]),
        ("hid", hid),
        ("pre", halves(g_pre)),
        ("ffn", halves(g_ffn)),
        ("act", act),
        ("att", att),
        ("branch", halves(g_branch)),
        ("tok", tok),
        ("qkv", halves(g_qkv)),
    )
    arrived = {}
    for i, (name, source) in enumerate(sources):
        copy = pltpu.make_async_remote_copy(
            src_ref=source,
            dst_ref=pair[name],
            send_sem=pair_send.at[i],
            recv_sem=pair_recv.at[i],
            device_id=core,
            device_id_type=MESH,
        )
        copy.start()
        arrived[name] = copy

    factors = {
        "up": (hid, "hid", g_pre, "pre"),
        "down": (act, "act", g_ffn, "ffn"),
        "output": (att, "att", g_branch, "branch"),
        "joint": (tok, "tok", g_qkv, "qkv"),
    }

    chunks = []
    todo = [("small", 128, 1)] + list(plan(model, g_qkv.shape[1], g_pre.shape[1]))
    at = 0
    for name, w, count in todo:
        for k in range(count):
            part = parts[name]
            r = part.shape[0] // chips
            chunks.append(Chunk(part, k * w, r, w, name, rest[5 * at : 5 * at + 5], at))
            at += 1

    def product(name, columns, w):
        left, left_pair, right, right_pair = factors[name]
        for item in (left_pair, right_pair):
            if item in arrived:
                arrived.pop(item).wait_recv()
        own = right[:, pl.ds(pl.multiple_of(c * (right.shape[1] // 2) + columns, 128), w)]
        other = pair[right_pair][:, columns : columns + w]
        dims = (((0,), (0,)), ((), ()))
        tile = 256

        @pl.loop(0, left.shape[1] // tile)
        def _(i):
            rows = pl.ds(pl.multiple_of(i * tile, tile), tile)
            total = lax.dot_general(left[:, rows], own, dims, preferred_element_type=f32)
            total += lax.dot_general(
                pair[left_pair][:, rows], other, dims, preferred_element_type=f32
            )
            parts[name][rows, columns : columns + w] = total.astype(bf16)

    def block(chunk, zb, pb, sb):
        (_, step_p), (_, step_s), _, _ = routes[chunk.kind == "small"]
        q = 4 * zb + step_p * pb + step_s * sb
        rows = pl.ds(pl.multiple_of(q * chunk.r, min(chunk.r, 16)), chunk.r)
        return chunk.part.at[rows, pl.ds(chunk.first, chunk.w)]

    def start(source, target, chunk, stage, device):
        pltpu.make_async_remote_copy(
            src_ref=source,
            dst_ref=target,
            send_sem=send.at[chunk.sems, stage],
            recv_sem=recv.at[chunk.sems, stage],
            device_id=device,
            device_id_type=MESH,
        ).start()

    def done(sems, chunk, stage, ref):
        pltpu.make_async_copy(ref, ref, sems.at[chunk.sems, stage]).wait()

    def places(chunk):
        (p, _), (s, _), first, second = routes[chunk.kind == "small"]
        return p, s, first, second

    made = set()

    def stage_0(chunk):
        if chunk.kind == "small":
            arrived.pop("small").wait_recv()
            chunk.part[...] = (small[:, c] + pair["small"][...]).reshape(chunk.part.shape)
        elif chunk.kind == "down":
            if "down" not in made:
                made.add("down")
                product("down", 0, chunk.part.shape[1])
        else:
            product(chunk.kind, chunk.first, chunk.w)
        p, _, first, _ = places(chunk)
        for zb in range(depth):
            for sb in range(2):
                start(block(chunk, zb, 1 - p, sb), chunk.b1.at[2 * zb + sb], chunk, 0, first)

    def stage_1(chunk):
        p, s, _, second = places(chunk)
        done(recv, chunk, 0, chunk.b1)
        for zb in range(depth):
            for sb in range(2):
                i = 2 * zb + sb
                total = chunk.b1[i].astype(f32) + block(chunk, zb, p, sb)[...].astype(f32)
                chunk.b1[i] = total.astype(chunk.b1.dtype)
        for zb in range(depth):
            start(chunk.b1.at[2 * zb + 1 - s], chunk.b2.at[zb], chunk, 1, second)

    def stage_2(chunk):
        _, s, _, _ = places(chunk)
        done(recv, chunk, 1, chunk.b2)
        for zb in range(depth):
            total = chunk.b2[zb].astype(f32) + chunk.b1[2 * zb + s].astype(f32)
            chunk.b2[zb] = total.astype(chunk.b2.dtype)
        for k in range(1, depth):
            start(chunk.b2.at[(z + k) % depth], chunk.b3.at[z], chunk, 2, along(k))
        chunk.b3[z] = chunk.b2[z]

    def stage_3(chunk):
        done(recv, chunk, 2, chunk.b3.at[pl.ds(0, depth - 1)])
        total = chunk.b3[0].astype(f32)
        for k in range(1, depth):
            total += chunk.b3[k].astype(f32)
        if chunk.kind == "small":
            outs["small"][...] = total
            return
        chunk.fin[...] = total
        half = chunk.r // 2
        start(chunk.fin.at[pl.ds(pl.multiple_of((1 - c) * half, 8), half)], chunk.got, chunk, 3, core)

    def stage_4(chunk):
        if chunk.kind == "small":
            return
        done(recv, chunk, 3, chunk.got)
        out = outs[chunk.kind]
        width = out.shape[1] // 2
        half = chunk.r // 2

        def columns(side):
            return pl.ds(pl.multiple_of(side * width + chunk.first, 128), chunk.w)

        out[:, columns(c)] = chunk.fin[pl.ds(pl.multiple_of(c * half, 8), half), :]
        out[:, columns(1 - c)] = chunk.got[...]

    stages = ((stage_0, 0), (stage_1, 2), (stage_2, 3), (stage_3, 4), (stage_4, 5))
    for step in range(len(chunks) + 5):
        for stage, lag in stages:
            if 0 <= step - lag < len(chunks):
                stage(chunks[step - lag])

    for i, (name, source) in enumerate(sources):
        pltpu.make_async_copy(pair[name], pair[name], pair_send.at[i]).wait()
    for chunk in chunks:
        done(send, chunk, 0, chunk.b1)
        done(send, chunk, 1, chunk.b2)
        done(send, chunk, 2, chunk.b3.at[pl.ds(0, depth - 1)])
        if chunk.kind != "small":
            done(send, chunk, 3, chunk.got)


def scatter_gradients(chips, tok, att, hid, act, g_qkv, g_branch, g_pre, g_ffn, small):
    rows, model = tok.shape
    devices = 2 * chips
    joint, up = g_qkv.shape[1], g_pre.shape[1]
    halved = {"qkv": joint // 2, "branch": model // 2, "pre": up // 2, "ffn": model // 2}
    scratch = [
        pltpu.VMEM((rows, model), bf16),
        pltpu.VMEM((rows, model), bf16),
        pltpu.VMEM((rows, model), bf16),
        pltpu.VMEM((rows, up), bf16),
        pltpu.VMEM((rows, halved["qkv"]), bf16),
        pltpu.VMEM((rows, halved["branch"]), bf16),
        pltpu.VMEM((rows, halved["pre"]), bf16),
        pltpu.VMEM((rows, halved["ffn"]), bf16),
        pltpu.VMEM((chips, 8, 128), f32),
    ]
    sizes = {
        "up": (model, up // 2, bf16),
        "down": (up, model // 2, bf16),
        "output": (model, model // 2, bf16),
        "joint": (model, joint // 2, bf16),
        "small": (chips * 8, 128, f32),
    }
    scratch += [pltpu.VMEM(sizes[k][:2], sizes[k][2]) for k in ("up", "down", "output", "joint", "small")]
    todo = [("small", 128, 1)] + list(plan(model, joint, up))
    count = sum(n for _, _, n in todo)
    scratch += [
        pltpu.SemaphoreType.DMA((9,)),
        pltpu.SemaphoreType.DMA((9,)),
        pltpu.SemaphoreType.DMA((count, 4)),
        pltpu.SemaphoreType.DMA((count, 4)),
    ]
    depth = chips // 4
    for name, w, n in todo:
        r, kind = sizes[name][0] // chips, sizes[name][2]
        for _ in range(n):
            scratch += [
                pltpu.VMEM((2 * depth, r, w), kind),
                pltpu.VMEM((depth, r, w), kind),
                pltpu.VMEM((depth, r, w), kind),
                pltpu.VMEM((r, w), f32),
                pltpu.VMEM((max(r // 2, 8), w), f32),
            ]
    vmem = pl.BlockSpec(memory_space=pltpu.VMEM)
    return pl.pallas_call(
        functools.partial(scatter_kernel, chips, model),
        out_shape=(
            jax.ShapeDtypeStruct((model // devices, joint), f32),
            jax.ShapeDtypeStruct((model // devices, model), f32),
            jax.ShapeDtypeStruct((model // devices, up), f32),
            jax.ShapeDtypeStruct((up // devices, model), f32),
            jax.ShapeDtypeStruct((8, 128), f32),
        ),
        in_specs=[vmem] * 9,
        out_specs=(vmem,) * 5,
        scratch_shapes=scratch,
        compiler_params=pltpu.CompilerParams(
            collective_id=0, has_side_effects=True, vmem_limit_bytes=60 << 20
        ),
        name="scatter_gradients",
    )(tok, att, hid, act, g_qkv, g_branch, g_pre, g_ffn, small)


def on_device(
    tokens,
    lengths,
    joint_weight,
    joint_bias,
    output_weight,
    output_bias,
    first_gain,
    first_shift,
    up_weight,
    up_bias,
    down_weight,
    down_bias,
    second_gain,
    second_shift,
    feature_matrix,
    cotangent,
):
    model = tokens.shape[1]
    heads, _, size = feature_matrix.shape
    both = ("dp", "feat")
    row_lengths = lax.dynamic_index_in_dim(lengths, lax.axis_index("dp"), 0, keepdims=False)
    valid = (row_lengths[0] > 0).astype(f32)
    features = lax.all_gather(feature_matrix, "feat", axis=1, tiled=True)
    qkv = (mm("td,de->te", tokens, joint_weight) + joint_bias).astype(bf16)
    attention, saved = attention_forward(qkv, features, valid, heads, size)
    branch_attn = mm("td,de->te", attention, output_weight) + output_bias
    wide = tokens.astype(f32)
    normal_1, inv_1 = layer_norm_parts(wide + branch_attn)
    hidden = normal_1 * first_gain + first_shift
    hidden_low = hidden.astype(bf16)
    pre = mm("td,df->tf", hidden_low, up_weight) + up_bias
    half_erf = 0.5 * (1.0 + lax.erf(pre * (0.5**0.5)))
    slope = half_erf + pre * jnp.exp(-0.5 * pre * pre) * 0.3989422804014327
    activated = (pre * half_erf).astype(bf16)
    branch_ffn = mm("tf,fd->td", activated, down_weight) + down_bias
    normal_2, inv_2 = layer_norm_parts(hidden + branch_ffn)
    layer_output = ((normal_2 * second_gain + second_shift) * valid).astype(bf16)
    moments = valid * jnp.stack(
        [jnp.sum(wide * wide), jnp.sum(branch_attn * branch_attn), jnp.sum(branch_ffn * branch_ffn)]
    )
    g_out = cotangent.astype(f32) * valid
    grad_secondgain = jnp.sum(g_out * normal_2, 0)
    grad_secondshift = jnp.sum(g_out, 0)
    g_second = layer_norm_back(g_out, normal_2, inv_2, second_gain)
    g_ffn = g_second.astype(bf16)
    grad_downbias = jnp.sum(g_ffn.astype(f32), 0)
    g_pre = (mm("td,fd->tf", g_ffn, down_weight) * slope).astype(bf16)
    grad_upbias = jnp.sum(g_pre.astype(f32), 0)
    g_hidden = g_second + mm("tf,df->td", g_pre, up_weight)
    grad_firstgain = jnp.sum(g_hidden * normal_1, 0)
    grad_firstshift = jnp.sum(g_hidden, 0)
    g_first = layer_norm_back(g_hidden, normal_1, inv_1, first_gain)
    g_branch = g_first.astype(bf16)
    grad_outputbias = jnp.sum(g_branch.astype(f32), 0)
    g_att = mm("te,de->td", g_branch, output_weight)
    g_qkv = attention_backward(g_att, saved, features, valid, heads, size)
    grad_jointbias = jnp.sum(g_qkv.astype(f32), 0)
    input_gradient = g_first + mm("te,de->td", g_qkv, joint_weight)

    shards = lax.axis_size(both)
    each = model // shards
    widths = (3 * each, each, each, each, up_bias.shape[0] // shards, each, each, each, 3)
    small = jnp.concatenate(
        [
            p.reshape(shards, -1)
            for p in (
                grad_jointbias,
                grad_outputbias,
                grad_firstgain,
                grad_firstshift,
                grad_upbias,
                grad_downbias,
                grad_secondgain,
                grad_secondshift,
            )
        ]
        + [jnp.broadcast_to(moments, (shards, 3))],
        axis=1,
    )
    if lax.axis_size("feat") == 4 and lax.axis_size("dp") == 8 and sum(widths) <= 1024:
        chips = shards // 2
        packed = jnp.pad(small, ((0, 0), (0, 1024 - sum(widths)))).reshape(chips, 2, 8, 128)
        *big, small = scatter_gradients(
            chips, tokens, attention, hidden_low, activated, g_qkv, g_branch, g_pre, g_ffn, packed
        )
        small = small.reshape(-1)
    else:
        small = lax.psum_scatter(small, both, scatter_dimension=0, tiled=True)[0]
        pairs = (
            ("td,te->de", tokens, g_qkv),
            ("td,te->de", attention, g_branch),
            ("td,tf->df", hidden_low, g_pre),
            ("tf,td->fd", activated, g_ffn),
        )
        big = [
            lax.psum_scatter(
                mm(spec, left, right).astype(bf16), both, scatter_dimension=0, tiled=True
            ).astype(f32)
            for spec, left, right in pairs
        ]
    cuts, at = [], 0
    for width in widths:
        cuts.append(small[at : at + width])
        at += width

    valid_count = jnp.sum(lengths).astype(f32)
    token_moments = jnp.sqrt(cuts[8] / (valid_count * model))
    return (
        layer_output,
        input_gradient,
        big[0],
        cuts[0],
        big[1],
        cuts[1],
        cuts[2],
        cuts[3],
        big[2],
        cuts[4],
        big[3],
        cuts[5],
        cuts[6],
        cuts[7],
        token_moments,
    )


def solution(mesh):
    rows = P(("dp", "feat"), None)
    flat = P(("dp", "feat"))
    in_specs = (rows,) + (P(),) * 13 + (P(None, "feat", None), rows)
    out_specs = (rows, rows, rows, flat, rows, flat, flat, flat, rows, flat, rows, flat, flat, flat, P())
    return jax.shard_map(
        on_device, mesh=mesh, in_specs=in_specs, out_specs=out_specs, check_vma=False
    )
```

```python
import functools

import jax
import jax.numpy as jnp
from jax import lax
from jax.experimental import pallas as pl
from jax.experimental.pallas import tpu as pltpu
from jax.sharding import PartitionSpec as P

epsilon = 1e-06
f32 = jnp.float32
bf16 = jnp.bfloat16


def mm(spec, a, b):
    return jnp.einsum(spec, a, b, preferred_element_type=f32)


def layer_norm_parts(v):
    center = v - jnp.mean(v, -1, keepdims=True)
    inv = lax.rsqrt(jnp.mean(center * center, -1, keepdims=True) + epsilon)
    return center * inv, inv


def layer_norm_back(grad, normal, inv, gain):
    scaled = grad * gain
    return inv * (
        scaled
        - jnp.mean(scaled, -1, keepdims=True)
        - normal * jnp.mean(scaled * normal, -1, keepdims=True)
    )


def attention_forward(qkv, features, valid, heads, size):
    rows = qkv.shape[0]
    model = heads * size
    scale = size ** (-0.25)
    norm = features.shape[1] ** (-0.5)
    q, k, v = (
        qkv[:, i * model : (i + 1) * model].reshape(rows, heads, size).transpose(1, 0, 2)
        for i in range(3)
    )
    qw, kw = q.astype(f32), k.astype(f32)
    q_shift = scale * mm("htd,hmd->htm", q, features) - (
        scale * scale / 2 * jnp.sum(qw * qw, -1, keepdims=True)
    )
    k_shift = scale * mm("htd,hmd->htm", k, features) - (
        scale * scale / 2 * jnp.sum(kw * kw, -1, keepdims=True)
    )
    q_top = jnp.max(q_shift, -1, keepdims=True)
    k_top = lax.pmax(jnp.max(k_shift, axis=(1, 2)), "feat")[:, None, None]
    q_raw = jnp.exp(q_shift - q_top) * norm
    k_raw = jnp.exp(k_shift - k_top) * norm * valid
    q_feat, k_feat = q_raw.astype(bf16), k_raw.astype(bf16)
    state = lax.psum(mm("htm,htd->hmd", k_feat, v), "feat").astype(bf16)
    totals = lax.psum(jnp.sum(k_feat.astype(f32), 1), "feat")
    numer = mm("htm,hmd->htd", q_feat, state) * valid
    denom = jnp.sum(q_feat.astype(f32) * totals[:, None, :], -1, keepdims=True) * valid
    safe = denom + (1.0 - valid)
    attention = (numer / safe).astype(bf16).transpose(1, 0, 2).reshape(rows, model)
    return attention, (q, k, v, q_raw, k_raw, state, totals, numer, safe)


def attention_backward(g_att, saved, features, valid, heads, size):
    q, k, v, q_raw, k_raw, state, totals, numer, safe = saved
    rows = g_att.shape[0]
    scale = size ** (-0.25)
    g_att = g_att.reshape(rows, heads, size).transpose(1, 0, 2)
    q_feat, k_feat = q_raw.astype(bf16), k_raw.astype(bf16)
    g_num = (g_att / safe * valid).astype(bf16)
    g_den = (-jnp.sum(g_att * numer, -1, keepdims=True) / (safe * safe) * valid).astype(bf16)
    g_den = g_den.astype(f32)
    g_state = lax.psum(mm("htm,htd->hmd", q_feat, g_num), "feat").astype(bf16)
    g_totals = lax.psum(jnp.sum(q_feat.astype(f32) * g_den, 1), "feat")
    g_aq = (mm("htd,hmd->htm", g_num, state) + g_den * totals[:, None, :]) * q_raw
    g_ak = (mm("htd,hmd->htm", v, g_state) + g_totals[:, None, :]) * k_raw
    g_v = mm("htm,hmd->htd", k_feat, g_state)

    def back(g_a, x):
        return scale * mm("htm,hmd->htd", g_a.astype(bf16), features) - (
            scale * scale * x.astype(f32) * jnp.sum(g_a, -1, keepdims=True)
        )

    parts = [back(g_aq, q), back(g_ak, k), g_v]
    return jnp.concatenate(
        [p.astype(bf16).transpose(1, 0, 2).reshape(rows, heads * size) for p in parts], axis=1
    )


MESH = pl.DeviceIdType.MESH


class Chunk:
    def __init__(self, part, first, r, w, kind, bufs, sems):
        self.part, self.first, self.r, self.w, self.kind = part, first, r, w, kind
        self.b1, self.b2, self.b3, self.fin, self.got = bufs
        self.sems = sems


def plan(tokens, joint, up):
    half_joint, half_up, half = joint // 2, up // 2, tokens // 2
    return (
        ("up", half_up // 3, 3),
        ("down", half // 3, 3),
        ("output", half, 1),
        ("joint", half_joint // 3, 3),
    )


def scatter_kernel(chips, model, *refs):
    (tok, att, hid, act, g_branch, g_pre, g_ffn) = refs[:7]
    (qkv, phi_q, phi_k, state, totals, safe, feats, joint_weight, output_weight, g_first) = refs[7:17]
    row_sums = refs[17:25]
    outs = dict(zip(("joint", "output", "up", "down", "small", "moments", "input"), refs[25:32]))
    scratch = list(refs[32:])
    pair = dict(zip(("tok", "att", "hid", "act", "qkv", "branch", "pre", "ffn"), scratch[:8]))
    parts = dict(zip(("up", "down", "output", "joint"), scratch[8:12]))
    pair_send, pair_recv, send, recv, small_send, small_recv = scratch[12:18]
    sums, near_sums, far_sums = scratch[18:21]
    (g_qkv, g_att, g_part, near_part, g_sum, far_part, g_state, g_totals, g_totals_parts) = scratch[21:30]
    state_send, state_recv = scratch[30:32]
    rest = scratch[32:]

    dp, feat = lax.axis_index("dp"), lax.axis_index("feat")
    depth = chips // 4
    z, x, y, c = dp // 2, dp % 2, feat // 2, feat % 2
    core = (dp, y * 2 + 1 - c)

    def route(turn):
        return (
            (x + turn * (y - x), 2 - turn),
            (y + turn * (x - y), 1 + turn),
            (z * 2 + x + (1 - turn) * (1 - 2 * x), (y + turn * (1 - 2 * y)) * 2 + c),
            (z * 2 + x + turn * (1 - 2 * x), (y + (1 - turn) * (1 - 2 * y)) * 2 + c),
        )

    (p, step_p), (s, step_s), first, second = route(c)

    def along(k):
        return ((z + k) % depth * 2 + x, feat)

    barrier = pltpu.get_barrier_semaphore()
    greeted = [core, first, second] + [along(k) for k in range(1, depth)]
    far_feat, cross_feat = (1 - y) * 2 + c, (1 - y) * 2 + 1 - c
    greeted.append((dp, cross_feat))
    for device in greeted:
        pl.semaphore_signal(barrier, inc=1, device_id=device, device_id_type=MESH)
    pl.semaphore_wait(barrier, len(greeted))

    def halves(ref):
        width = ref.shape[1] // 2
        return ref.at[:, pl.ds(pl.multiple_of((1 - c) * width, 128), width)]

    sources = (
        ("hid", hid),
        ("pre", halves(g_pre)),
        ("ffn", halves(g_ffn)),
        ("act", act),
        ("att", att),
        ("branch", halves(g_branch)),
        ("tok", tok),
        ("qkv", halves(g_qkv)),
    )
    arrived = {}

    def swap(names):
        for i, (name, source) in enumerate(sources):
            if name in names:
                copy = pltpu.make_async_remote_copy(
                    src_ref=source,
                    dst_ref=pair[name],
                    send_sem=pair_send.at[i],
                    recv_sem=pair_recv.at[i],
                    device_id=core,
                    device_id_type=MESH,
                )
                copy.start()
                arrived[name] = copy

    swap(("hid", "pre", "ffn", "act", "att", "branch", "tok"))

    factors = {
        "up": (hid, "hid", g_pre, "pre"),
        "down": (act, "act", g_ffn, "ffn"),
        "output": (att, "att", g_branch, "branch"),
        "joint": (tok, "tok", g_qkv, "qkv"),
    }

    chunks = []
    at = 0
    for name, w, count in plan(model, g_qkv.shape[1], g_pre.shape[1]):
        for k in range(count):
            part = parts[name]
            r = part.shape[0] // chips
            chunks.append(Chunk(part, k * w, r, w, name, rest[5 * at : 5 * at + 5], at))
            at += 1

    def product(name, columns, w):
        left, left_pair, right, right_pair = factors[name]
        for item in (left_pair, right_pair):
            if item in arrived:
                arrived.pop(item).wait_recv()
        own = right[:, pl.ds(pl.multiple_of(c * (right.shape[1] // 2) + columns, 128), w)]
        other = pair[right_pair][:, columns : columns + w]
        dims = (((0,), (0,)), ((), ()))
        tile = 256

        @pl.loop(0, left.shape[1] // tile)
        def _(i):
            rows = pl.ds(pl.multiple_of(i * tile, tile), tile)
            total = lax.dot_general(left[:, rows], own, dims, preferred_element_type=f32)
            total += lax.dot_general(
                pair[left_pair][:, rows], other, dims, preferred_element_type=f32
            )
            parts[name][rows, columns : columns + w] = total.astype(bf16)

    def block(chunk, zb, pb, sb):
        q = 4 * zb + step_p * pb + step_s * sb
        rows = pl.ds(pl.multiple_of(q * chunk.r, min(chunk.r, 16)), chunk.r)
        return chunk.part.at[rows, pl.ds(chunk.first, chunk.w)]

    def start(source, target, chunk, stage, device):
        pltpu.make_async_remote_copy(
            src_ref=source,
            dst_ref=target,
            send_sem=send.at[chunk.sems, stage],
            recv_sem=recv.at[chunk.sems, stage],
            device_id=device,
            device_id_type=MESH,
        ).start()

    def done(sems, chunk, stage, ref):
        pltpu.make_async_copy(ref, ref, sems.at[chunk.sems, stage]).wait()

    made = set()

    def stage_0(chunk):
        if chunk.kind == "down":
            if "down" not in made:
                made.add("down")
                product("down", 0, chunk.part.shape[1])
        else:
            product(chunk.kind, chunk.first, chunk.w)
        for zb in range(depth):
            for sb in range(2):
                start(block(chunk, zb, 1 - p, sb), chunk.b1.at[2 * zb + sb], chunk, 0, first)

    def stage_1(chunk):
        done(recv, chunk, 0, chunk.b1)
        for zb in range(depth):
            for sb in range(2):
                i = 2 * zb + sb
                total = chunk.b1[i].astype(f32) + block(chunk, zb, p, sb)[...].astype(f32)
                chunk.b1[i] = total.astype(chunk.b1.dtype)
        for zb in range(depth):
            start(chunk.b1.at[2 * zb + 1 - s], chunk.b2.at[zb], chunk, 1, second)

    def stage_2(chunk):
        done(recv, chunk, 1, chunk.b2)
        for zb in range(depth):
            total = chunk.b2[zb].astype(f32) + chunk.b1[2 * zb + s].astype(f32)
            chunk.b2[zb] = total.astype(chunk.b2.dtype)
        for k in range(1, depth):
            start(chunk.b2.at[(z + k) % depth], chunk.b3.at[z], chunk, 2, along(k))
        chunk.b3[z] = chunk.b2[z]

    def stage_3(chunk):
        done(recv, chunk, 2, chunk.b3.at[pl.ds(0, depth - 1)])
        total = chunk.b3[0].astype(f32)
        for k in range(1, depth):
            total += chunk.b3[k].astype(f32)
        chunk.fin[...] = total
        half = chunk.r // 2
        start(chunk.fin.at[pl.ds(pl.multiple_of((1 - c) * half, 8), half)], chunk.got, chunk, 3, core)

    def stage_4(chunk):
        done(recv, chunk, 3, chunk.got)
        out = outs[chunk.kind]
        width = out.shape[1] // 2
        half = chunk.r // 2

        def columns(side):
            return pl.ds(pl.multiple_of(side * width + chunk.first, 128), chunk.w)

        out[:, columns(c)] = chunk.fin[pl.ds(pl.multiple_of(c * half, 8), half), :]
        out[:, columns(1 - c)] = chunk.got[...]

    _, _, along_x, along_y = route(0)

    def small_step(k):
        if k == 0:
            sums[0] = jnp.zeros(sums.shape[1:], f32)
            sums[0, 0:1, 0 : g_qkv.shape[1]] = jnp.sum(
                g_qkv[...].astype(f32), axis=0, keepdims=True
            )
            for i, source in enumerate(row_sums[:7]):
                sums[0, i + 1 : i + 2, 0 : source.shape[1]] = source[...]
            sums[0, 1:2, sums.shape[2] - 128 :] = row_sums[7][...]
        elif k < 4:
            arrive = pltpu.make_async_copy(near_sums.at[k - 1], near_sums.at[k - 1], small_recv.at[k - 1])
            arrive.wait()
            sums[k] = sums[k - 1] + near_sums[k - 1]
        if k < 3:
            targets = [(near_sums.at[k], (core, along_x, along_y)[k])]
        elif k == 3:
            targets = [(far_sums.at[z], along(j)) for j in range(1, depth)]
        else:
            waited = far_sums.at[pl.ds(0, depth - 1)]
            pltpu.make_async_copy(waited, waited, small_recv.at[3]).wait()
            total = far_sums[0]
            for j in range(1, depth):
                total += far_sums[j]
            outs["moments"][...] = total[:, total.shape[1] - 128 :]
            width = total.shape[1]
            place = dp * 4 + feat
            turned = {}
            for i, source in enumerate((g_qkv, *row_sums[:7])):
                own = source.shape[1] // (2 * chips)
                if own not in turned:
                    turned[own] = pltpu.roll(total, (width - own * place) % width, 1)[:, :128]
                outs["small"][i : i + 1, :] = turned[own][i : i + 1, :]
            return
        for target, device in targets:
            pltpu.make_async_remote_copy(
                src_ref=sums.at[k],
                dst_ref=target,
                send_sem=small_send.at[k],
                recv_sem=small_recv.at[k],
                device_id=device,
                device_id_type=MESH,
            ).start()
        if k == 3:
            far_sums[z] = sums[3]

    rows = tok.shape[0]
    pairs, count, lanes = feats.shape
    size = lanes // 2
    scale = size ** (-0.25)
    half = pairs // 2
    mine, theirs = c * half, (1 - c) * half
    lane = lax.broadcasted_iota(jnp.int32, (rows, lanes), 1)
    state_row = lax.broadcasted_iota(jnp.int32, (lanes, count), 0)

    def own_half(value, b):
        return jnp.where(lane // size == b, value, jnp.zeros_like(value))

    def either(values):
        return jnp.where(lane < size, values[0], values[1])

    def of_head(h):
        return pl.ds(pl.multiple_of(h * count, count), count)

    def of_pair(base, i):
        return pl.ds(pl.multiple_of(base * model + i * lanes, lanes), lanes)

    def to_inputs(grads, base, i):
        inputs = qkv[:, of_pair(base, i)].astype(f32)
        results = []
        for grad in grads:
            linear = scale * jnp.dot(grad.astype(bf16), feats[i], preferred_element_type=f32)
            results.append(linear - scale * scale * inputs * jnp.sum(grad, -1, keepdims=True))
        g_qkv[:, of_pair(base, i)] = either(results).astype(bf16)

    def query_back(i):
        grad = g_att[:, of_pair(0, i)]
        ratio = grad * att[:, of_pair(0, i)].astype(f32)
        tops, dens = [], []
        for b in range(2):
            top = 1.0 / jnp.sum(jnp.where(lane == 2 * i + b, safe[...], 0.0), -1, keepdims=True)
            tops.append(top)
            den = -jnp.sum(own_half(ratio, b), -1, keepdims=True) * top
            dens.append(den.astype(bf16).astype(f32))
        numer = (grad * either(tops)).astype(bf16)
        products, logits = [], []
        for b in range(2):
            h = 2 * i + b
            low = phi_q[:, of_head(h)]
            wide = low.astype(f32)
            products.append(dot(numer, low, 0, 0))
            g_totals_parts[feat, pl.ds(h, 1), :] = jnp.sum(wide * dens[b], axis=0, keepdims=True)
            back = jnp.dot(own_half(numer, b), state[i], preferred_element_type=f32)
            logits.append((back + dens[b] * totals[pl.ds(h, 1), :]) * wide)
        g_part[i] = jnp.where(state_row < size, products[0], products[1]).astype(bf16)
        to_inputs(logits, 0, i)

    def key_back(i):
        values = qkv[:, of_pair(2, i)]
        held = g_state[i]
        logits, g_values = [], []
        for b in range(2):
            h = 2 * i + b
            low = phi_k[:, of_head(h)]
            back = jnp.dot(own_half(values, b), held, preferred_element_type=f32)
            logits.append((back + g_totals[pl.ds(h, 1), :]) * low.astype(f32))
            g_values.append(dot(low, held, 1, 1))
        g_qkv[:, of_pair(2, i)] = either(g_values).astype(bf16)
        to_inputs(logits, 1, i)

    def state_copy(source, target, i, other):
        copy = pltpu.make_async_remote_copy(
            src_ref=source,
            dst_ref=target,
            send_sem=state_send.at[i],
            recv_sem=state_recv.at[i],
            device_id=(dp, other),
            device_id_type=MESH,
        )
        copy.start()
        return copy

    moved = {}

    def attention_a():
        g_totals_parts[feat] = jnp.zeros(g_totals_parts.shape[1:], f32)
        tile = 256

        @pl.loop(0, model // tile)
        def _(i):
            own = pl.ds(pl.multiple_of(i * tile, tile), tile)
            g_att[:, own] = dot(g_branch[...], output_weight[own, :], 1, 1)

        @pl.loop(0, half)
        def _(j):
            query_back(theirs + j)

        moved["near"] = state_copy(g_part.at[pl.ds(theirs, half)], near_part, 0, y * 2 + 1 - c)

    def attention_b():
        @pl.loop(0, half)
        def _(j):
            query_back(mine + j)

        for other in (y * 2 + 1 - c, far_feat, cross_feat):
            state_copy(g_totals_parts.at[feat], g_totals_parts.at[feat], 1, other)
        moved["near"].wait_recv()
        g_sum[...] = (g_part[pl.ds(mine, half)].astype(f32) + near_part[...].astype(f32)).astype(bf16)
        moved["far"] = state_copy(g_sum, far_part, 2, far_feat)

    three_totals = g_totals_parts.at[pl.ds(0, 3)]

    def attention_c():
        moved["far"].wait_recv()
        own = pl.ds(mine, half)
        g_state[own] = (g_sum[...].astype(f32) + far_part[...].astype(f32)).astype(bf16)
        moved["back"] = state_copy(g_state.at[own], g_state.at[own], 3, y * 2 + 1 - c)
        pltpu.make_async_copy(three_totals, three_totals, state_recv.at[1]).wait()
        g_totals[...] = (g_totals_parts[0] + g_totals_parts[1]) + (g_totals_parts[2] + g_totals_parts[3])

        @pl.loop(0, half)
        def _(j):
            key_back(mine + j)

    def attention_d():
        moved["back"].wait_recv()

        @pl.loop(0, half)
        def _(j):
            key_back(theirs + j)

        swap(("qkv",))

    def attention_e():
        tile = 256

        @pl.loop(0, model // tile)
        def _(i):
            own = pl.ds(pl.multiple_of(i * tile, tile), tile)
            outs["input"][:, own] = g_first[:, own] + dot(g_qkv[...], joint_weight[own, :], 1, 1)

    attention_steps = {
        0: attention_a,
        1: attention_b,
        3: attention_c,
        4: attention_d,
        5: attention_e,
    }

    stages = ((stage_0, 0), (stage_1, 2), (stage_2, 3), (stage_3, 4), (stage_4, 5))
    for step in range(len(chunks) + 5):
        for stage, lag in stages:
            if 0 <= step - lag < len(chunks):
                stage(chunks[step - lag])
        if 7 <= step <= 11:
            small_step(step - 7)
        if step in attention_steps:
            attention_steps[step]()

    for i, (name, source) in enumerate(sources):
        pltpu.make_async_copy(pair[name], pair[name], pair_send.at[i]).wait()
    for chunk in chunks:
        done(send, chunk, 0, chunk.b1)
        done(send, chunk, 1, chunk.b2)
        done(send, chunk, 2, chunk.b3.at[pl.ds(0, depth - 1)])
        done(send, chunk, 3, chunk.got)
    for made in moved.values():
        made.wait_send()
    pltpu.make_async_copy(three_totals, three_totals, state_send.at[1]).wait()
    for i in range(3):
        pltpu.make_async_copy(near_sums.at[i], near_sums.at[i], small_send.at[i]).wait()
    waited = far_sums.at[pl.ds(0, depth - 1)]
    pltpu.make_async_copy(waited, waited, small_send.at[3]).wait()


def scatter_gradients(chips, tok, att, hid, act, g_branch, g_pre, g_ffn, saved, weights, g_first, row_sums):
    rows, model = tok.shape
    devices = 2 * chips
    g_qkv, feats = saved[0], saved[-1]
    pairs, features, lanes = feats.shape
    joint, up = g_qkv.shape[1], g_pre.shape[1]
    halved = {"qkv": joint // 2, "branch": model // 2, "pre": up // 2, "ffn": model // 2}
    scratch = [
        pltpu.VMEM((rows, model), bf16),
        pltpu.VMEM((rows, model), bf16),
        pltpu.VMEM((rows, model), bf16),
        pltpu.VMEM((rows, up), bf16),
        pltpu.VMEM((rows, halved["qkv"]), bf16),
        pltpu.VMEM((rows, halved["branch"]), bf16),
        pltpu.VMEM((rows, halved["pre"]), bf16),
        pltpu.VMEM((rows, halved["ffn"]), bf16),
    ]
    sizes = {
        "up": (model, up // 2, bf16),
        "down": (up, model // 2, bf16),
        "output": (model, model // 2, bf16),
        "joint": (model, joint // 2, bf16),
    }
    scratch += [pltpu.VMEM(sizes[k][:2], sizes[k][2]) for k in ("up", "down", "output", "joint")]
    todo = plan(model, joint, up)
    count = sum(n for _, _, n in todo)
    scratch += [
        pltpu.SemaphoreType.DMA((8,)),
        pltpu.SemaphoreType.DMA((8,)),
        pltpu.SemaphoreType.DMA((count, 4)),
        pltpu.SemaphoreType.DMA((count, 4)),
        pltpu.SemaphoreType.DMA((4,)),
        pltpu.SemaphoreType.DMA((4,)),
    ]
    depth = chips // 4
    scratch += [
        pltpu.VMEM((4, 8, up), f32),
        pltpu.VMEM((3, 8, up), f32),
        pltpu.VMEM((depth, 8, up), f32),
        pltpu.VMEM((rows, joint), bf16),
        pltpu.VMEM((rows, model), f32),
        pltpu.VMEM((pairs, lanes, features), bf16),
        pltpu.VMEM((pairs // 2, lanes, features), bf16),
        pltpu.VMEM((pairs // 2, lanes, features), bf16),
        pltpu.VMEM((pairs // 2, lanes, features), bf16),
        pltpu.VMEM((pairs, lanes, features), bf16),
        pltpu.VMEM((16, features), f32),
        pltpu.VMEM((4, 16, features), f32),
        pltpu.SemaphoreType.DMA((4,)),
        pltpu.SemaphoreType.DMA((4,)),
    ]
    for name, w, n in todo:
        r, kind = sizes[name][0] // chips, sizes[name][2]
        for _ in range(n):
            scratch += [
                pltpu.VMEM((2 * depth, r, w), kind),
                pltpu.VMEM((depth, r, w), kind),
                pltpu.VMEM((depth, r, w), kind),
                pltpu.VMEM((r, w), f32),
                pltpu.VMEM((r // 2, w), f32),
            ]
    vmem = pl.BlockSpec(memory_space=pltpu.VMEM)
    return pl.pallas_call(
        functools.partial(scatter_kernel, chips, model),
        out_shape=(
            jax.ShapeDtypeStruct((model // devices, joint), f32),
            jax.ShapeDtypeStruct((model // devices, model), f32),
            jax.ShapeDtypeStruct((model // devices, up), f32),
            jax.ShapeDtypeStruct((up // devices, model), f32),
            jax.ShapeDtypeStruct((8, 128), f32),
            jax.ShapeDtypeStruct((8, 128), f32),
            jax.ShapeDtypeStruct((rows, model), f32),
        ),
        in_specs=[vmem] * 25,
        out_specs=(vmem,) * 7,
        scratch_shapes=scratch,
        compiler_params=pltpu.CompilerParams(
            collective_id=0, has_side_effects=True, vmem_limit_bytes=60 << 20
        ),
        name="scatter_gradients",
    )(tok, att, hid, act, g_branch, g_pre, g_ffn, *saved, *weights, g_first, *row_sums)


def dot(a, b, left, right):
    return lax.dot_general(a, b, (((left,), (right,)), ((), ())), preferred_element_type=f32)


def attention_kernel(*refs):
    (tok, weight, bias, shard, valid_ref) = refs[:5]
    (att, qkv, phi_q, phi_k, state, totals, safe, kept) = refs[5:13]
    (feats, shift, tops, part, pair_part, pair_sum, far_sum, part_totals) = refs[13:21]
    send, recv = refs[21:23]
    rows, model = tok.shape
    pairs, share, lanes = shard.shape
    size = lanes // 2
    count = feats.shape[1]
    heads = 2 * pairs
    scale = size ** (-0.25)
    norm = count ** (-0.5)
    dp, feat = lax.axis_index("dp"), lax.axis_index("feat")
    y, c = feat // 2, feat % 2
    core, far, cross = y * 2 + 1 - c, (1 - y) * 2 + c, (1 - y) * 2 + 1 - c
    others = (core, far, cross)

    barrier = pltpu.get_barrier_semaphore()
    for other in others:
        pl.semaphore_signal(barrier, inc=1, device_id=(dp, other), device_id_type=MESH)
    pl.semaphore_wait(barrier, 3)

    def copy(source, target, i, other):
        made = pltpu.make_async_remote_copy(
            src_ref=source,
            dst_ref=target,
            send_sem=send.at[i],
            recv_sem=recv.at[i],
            device_id=(dp, other),
            device_id_type=MESH,
        )
        made.start()
        return made

    def slot(owner):
        return feats.at[:, pl.ds(pl.multiple_of(owner * share, share), share), :]

    to_far = copy(shard, slot(feat), 0, far)
    to_core = copy(shard, slot(feat), 1, core)
    feats[:, pl.ds(pl.multiple_of(feat * share, share), share), :] = shard[...]

    tile = 256

    @pl.loop(0, qkv.shape[1] // tile)
    def _(i):
        columns = pl.ds(pl.multiple_of(i * tile, tile), tile)
        total = jnp.dot(tok[...], weight[:, columns], preferred_element_type=f32)
        qkv[:, columns] = (total + bias[:, columns]).astype(bf16)

    to_far.wait_recv()
    passed = copy(slot(far), slot(far), 2, core)
    to_core.wait_recv()
    passed.wait_recv()

    lane = lax.broadcasted_iota(jnp.int32, (rows, lanes), 1)
    row_lane = lax.broadcasted_iota(jnp.int32, (8, 128), 1)

    def pair_of(base, i):
        return qkv[:, pl.ds(pl.multiple_of(base * model + i * lanes, lanes), lanes)]

    def own_half(value, b):
        return jnp.where(lane // size == b, value, jnp.zeros_like(value))

    def of_head(h):
        return pl.ds(pl.multiple_of(h * count, count), count)

    def key_logits(i, top):
        keys = pair_of(1, i)
        for b in range(2):
            mine = own_half(keys, b)
            wide = mine.astype(f32)
            logits = scale * dot(mine, feats[i], 1, 1) - (
                scale * scale / 2 * jnp.sum(wide * wide, -1, keepdims=True)
            )
            shift[2 * i + b] = logits
            best = jnp.max(jnp.max(logits, axis=1, keepdims=True), axis=0, keepdims=True)
            top = jnp.where(row_lane == 2 * i + b, best, top)
        return top

    tops[feat] = lax.fori_loop(0, pairs, key_logits, jnp.full((8, 128), -1e30, f32))
    top_copies = [copy(tops.at[feat], tops.at[feat], 3, other) for other in others]

    @pl.loop(0, pairs)
    def _(i):
        queries = pair_of(0, i)
        for b in range(2):
            logits = scale * dot(own_half(queries, b), feats[i], 1, 1)
            raw = jnp.exp(logits - jnp.max(logits, -1, keepdims=True)) * norm
            phi_q[:, of_head(2 * i + b)] = raw.astype(bf16)

    three = tops.at[pl.ds(0, 3)]
    pltpu.make_async_copy(three, three, recv.at[3]).wait()
    top = jnp.maximum(jnp.maximum(tops[0], tops[1]), jnp.maximum(tops[2], tops[3]))
    valid = valid_ref[0, 0]
    state_row = lax.broadcasted_iota(jnp.int32, (lanes, count), 0)
    part_totals[feat] = jnp.zeros(part_totals.shape[1:], f32)

    def key_state(i):
        values = pair_of(2, i)
        products = []
        for b in range(2):
            h = 2 * i + b
            best = jnp.max(jnp.where(row_lane == h, top, -1e30), axis=1, keepdims=True)[:1]
            raw = (jnp.exp(shift[h] - best) * (norm * valid)).astype(bf16)
            phi_k[:, of_head(h)] = raw
            part_totals[feat, pl.ds(h, 1), :] = jnp.sum(raw.astype(f32), axis=0, keepdims=True)
            products.append(dot(values, raw, 0, 0))
        part[i] = jnp.where(state_row < size, products[0], products[1]).astype(bf16)

    half = pairs // 2
    mine, theirs = c * half, (1 - c) * half

    @pl.loop(0, half)
    def _(j):
        key_state(theirs + j)

    near = copy(part.at[pl.ds(theirs, half)], pair_part, 4, core)

    @pl.loop(0, half)
    def _(j):
        key_state(mine + j)

    for other in others:
        copy(part_totals.at[feat], part_totals.at[feat], 5, other)
    near.wait_recv()
    pair_sum[...] = (part[pl.ds(mine, half)].astype(f32) + pair_part[...].astype(f32)).astype(bf16)
    across = copy(pair_sum, far_sum, 6, far)
    across.wait_recv()
    state[pl.ds(mine, half)] = (pair_sum[...].astype(f32) + far_sum[...].astype(f32)).astype(bf16)
    back = copy(state.at[pl.ds(mine, half)], state.at[pl.ds(mine, half)], 7, core)
    three_totals = part_totals.at[pl.ds(0, 3)]
    pltpu.make_async_copy(three_totals, three_totals, recv.at[5]).wait()
    totals[...] = (part_totals[0] + part_totals[1]) + (part_totals[2] + part_totals[3])
    safe[...] = jnp.ones(safe.shape, f32)

    def attend(i):
        held = state[i]
        results = []
        for b in range(2):
            h = 2 * i + b
            feature = phi_q[:, of_head(h)]
            denom = jnp.sum(feature.astype(f32) * totals[pl.ds(h, 1), :], -1, keepdims=True)
            bottom = denom + (1.0 - valid)
            safe[...] = jnp.where(
                lax.broadcasted_iota(jnp.int32, safe.shape, 1) == h, bottom, safe[...]
            )
            results.append(dot(feature, held, 1, 1) / bottom)
        att[:, pl.ds(pl.multiple_of(i * lanes, lanes), lanes)] = jnp.where(
            lane < size, results[0], results[1]
        ).astype(bf16)

    @pl.loop(0, half)
    def _(j):
        attend(mine + j)

    back.wait_recv()

    @pl.loop(0, half)
    def _(j):
        attend(theirs + j)

    kept[...] = feats[...]
    for made in (to_far, to_core, passed, near, across, back):
        made.wait_send()
    pltpu.make_async_copy(three, three, send.at[3]).wait()
    pltpu.make_async_copy(three_totals, three_totals, send.at[5]).wait()


def attention_call(tokens, weight, bias, features, valid):
    rows, model = tokens.shape
    heads, share, size = features.shape
    count = share * 4
    pairs, lanes = heads // 2, 2 * size
    shard = features.reshape(pairs, 2, share, size).transpose(0, 2, 1, 3).reshape(pairs, share, lanes)
    vmem = pl.BlockSpec(memory_space=pltpu.VMEM)
    return pl.pallas_call(
        attention_kernel,
        out_shape=(
            jax.ShapeDtypeStruct((rows, model), bf16),
            jax.ShapeDtypeStruct((rows, 3 * model), bf16),
            jax.ShapeDtypeStruct((rows, heads * count), bf16),
            jax.ShapeDtypeStruct((rows, heads * count), bf16),
            jax.ShapeDtypeStruct((pairs, lanes, count), bf16),
            jax.ShapeDtypeStruct((16, count), f32),
            jax.ShapeDtypeStruct((rows, 128), f32),
            jax.ShapeDtypeStruct((pairs, count, lanes), bf16),
        ),
        in_specs=[vmem] * 4 + [pl.BlockSpec(memory_space=pltpu.SMEM)],
        out_specs=(vmem,) * 8,
        scratch_shapes=[
            pltpu.VMEM((pairs, count, lanes), bf16),
            pltpu.VMEM((heads, rows, count), f32),
            pltpu.VMEM((4, 8, 128), f32),
            pltpu.VMEM((pairs, lanes, count), bf16),
            pltpu.VMEM((pairs // 2, lanes, count), bf16),
            pltpu.VMEM((pairs // 2, lanes, count), bf16),
            pltpu.VMEM((pairs // 2, lanes, count), bf16),
            pltpu.VMEM((4, 16, count), f32),
            pltpu.SemaphoreType.DMA((8,)),
            pltpu.SemaphoreType.DMA((8,)),
        ],
        compiler_params=pltpu.CompilerParams(
            collective_id=1, has_side_effects=True, vmem_limit_bytes=40 << 20
        ),
        name="attention",
    )(tokens, weight, bias.reshape(1, -1), shard, valid.reshape(1, 1))


def finish_kernel(*refs):
    (count, joint, output, up, down, inputs, small, moments) = refs[:8]
    outs = refs[8:]
    for source, target in zip((joint, output, up, down, inputs), outs[:5]):
        target[...] = source[...]
    for i, target in enumerate(outs[5:13]):
        target[...] = small[i, 0 : target.shape[0]]
    outs[13][...] = jnp.sqrt(moments[1, 0:3] / count[0, 0])


def finish(count, big, small, moments, widths):
    vmem = pl.BlockSpec(memory_space=pltpu.VMEM)
    return pl.pallas_call(
        finish_kernel,
        out_shape=tuple(jax.ShapeDtypeStruct(b.shape, f32) for b in big)
        + tuple(jax.ShapeDtypeStruct((w,), f32) for w in widths),
        in_specs=[pl.BlockSpec(memory_space=pltpu.SMEM)] + [vmem] * 7,
        out_specs=(vmem,) * 14,
        name="finish",
    )(count.reshape(1, 1), *big, small, moments)


def on_device(
    tokens,
    lengths,
    joint_weight,
    joint_bias,
    output_weight,
    output_bias,
    first_gain,
    first_shift,
    up_weight,
    up_bias,
    down_weight,
    down_bias,
    second_gain,
    second_shift,
    feature_matrix,
    cotangent,
):
    model = tokens.shape[1]
    heads, _, size = feature_matrix.shape
    both = ("dp", "feat")
    row_lengths = lax.dynamic_index_in_dim(lengths, lax.axis_index("dp"), 0, keepdims=False)
    valid = (row_lengths[0] > 0).astype(f32)
    kernels = lax.axis_size("feat") == 4 and lax.axis_size("dp") == 8
    if kernels:
        attention, *saved = attention_call(tokens, joint_weight, joint_bias, feature_matrix, valid)
    else:
        features = lax.all_gather(feature_matrix, "feat", axis=1, tiled=True)
        qkv = (mm("td,de->te", tokens, joint_weight) + joint_bias).astype(bf16)
        attention, saved = attention_forward(qkv, features, valid, heads, size)
    branch_attn = mm("td,de->te", attention, output_weight) + output_bias
    wide = tokens.astype(f32)
    normal_1, inv_1 = layer_norm_parts(wide + branch_attn)
    hidden = normal_1 * first_gain + first_shift
    hidden_low = hidden.astype(bf16)
    pre = mm("td,df->tf", hidden_low, up_weight) + up_bias
    half_erf = 0.5 * (1.0 + lax.erf(pre * (0.5**0.5)))
    slope = half_erf + pre * jnp.exp(-0.5 * pre * pre) * 0.3989422804014327
    activated = (pre * half_erf).astype(bf16)
    branch_ffn = mm("tf,fd->td", activated, down_weight) + down_bias
    normal_2, inv_2 = layer_norm_parts(hidden + branch_ffn)
    layer_output = ((normal_2 * second_gain + second_shift) * valid).astype(bf16)
    moments = valid * jnp.stack(
        [jnp.sum(wide * wide), jnp.sum(branch_attn * branch_attn), jnp.sum(branch_ffn * branch_ffn)]
    )
    g_out = cotangent.astype(f32) * valid
    grad_secondgain = jnp.sum(g_out * normal_2, 0)
    grad_secondshift = jnp.sum(g_out, 0)
    g_second = layer_norm_back(g_out, normal_2, inv_2, second_gain)
    g_ffn = g_second.astype(bf16)
    grad_downbias = jnp.sum(g_ffn.astype(f32), 0)
    g_pre = (mm("td,fd->tf", g_ffn, down_weight) * slope).astype(bf16)
    grad_upbias = jnp.sum(g_pre.astype(f32), 0)
    g_hidden = g_second + mm("tf,df->td", g_pre, up_weight)
    grad_firstgain = jnp.sum(g_hidden * normal_1, 0)
    grad_firstshift = jnp.sum(g_hidden, 0)
    g_first = layer_norm_back(g_hidden, normal_1, inv_1, first_gain)
    g_branch = g_first.astype(bf16)
    grad_outputbias = jnp.sum(g_branch.astype(f32), 0)
    shards = lax.axis_size(both)
    each = model // shards
    widths = (3 * each, each, each, each, up_bias.shape[0] // shards, each, each, each, 3)
    row_sums = (
        grad_outputbias,
        grad_firstgain,
        grad_firstshift,
        grad_upbias,
        grad_downbias,
        grad_secondgain,
        grad_secondshift,
    )
    count = jnp.sum(lengths).astype(f32) * model
    if kernels:
        *big, small, moment_sums, inputs = scatter_gradients(
            shards // 2,
            tokens,
            attention,
            hidden_low,
            activated,
            g_branch,
            g_pre,
            g_ffn,
            saved,
            (joint_weight, output_weight),
            g_first,
            [p.reshape(1, -1) for p in row_sums] + [jnp.pad(moments, (0, 125)).reshape(1, 128)],
        )
        *big, input_gradient = big + [inputs]
        *big, input_gradient, s0, s1, s2, s3, s4, s5, s6, s7, token_moments = finish(
            count, [*big, input_gradient], small, moment_sums, widths
        )
        cuts = (s0, s1, s2, s3, s4, s5, s6, s7)
    else:
        g_att = mm("te,de->td", g_branch, output_weight)
        g_qkv = attention_backward(g_att, saved, features, valid, heads, size)
        input_gradient = g_first + mm("te,de->td", g_qkv, joint_weight)
        grad_jointbias = jnp.sum(g_qkv.astype(f32), 0)
        small = jnp.concatenate(
            [p.reshape(shards, -1) for p in (grad_jointbias, *row_sums)]
            + [jnp.broadcast_to(moments, (shards, 3))],
            axis=1,
        )
        small = lax.psum_scatter(small, both, scatter_dimension=0, tiled=True)[0]
        pairs = (
            ("td,te->de", tokens, g_qkv),
            ("td,te->de", attention, g_branch),
            ("td,tf->df", hidden_low, g_pre),
            ("tf,td->fd", activated, g_ffn),
        )
        big = [
            lax.psum_scatter(
                mm(spec, left, right).astype(bf16), both, scatter_dimension=0, tiled=True
            ).astype(f32)
            for spec, left, right in pairs
        ]
        cuts, at = [], 0
        for width in widths:
            cuts.append(small[at : at + width])
            at += width
        token_moments = jnp.sqrt(cuts[8] / count)
    return (
        layer_output,
        input_gradient,
        big[0],
        cuts[0],
        big[1],
        cuts[1],
        cuts[2],
        cuts[3],
        big[2],
        cuts[4],
        big[3],
        cuts[5],
        cuts[6],
        cuts[7],
        token_moments,
    )


def solution(mesh):
    rows = P(("dp", "feat"), None)
    flat = P(("dp", "feat"))
    in_specs = (rows,) + (P(),) * 13 + (P(None, "feat", None), rows)
    out_specs = (rows, rows, rows, flat, rows, flat, flat, flat, rows, flat, rows, flat, flat, flat, P())
    return jax.shard_map(
        on_device, mesh=mesh, in_specs=in_specs, out_specs=out_specs, check_vma=False
    )
```
